32 devices in a mesh: gx: 8 (over z, y), gy: 4 (over x, core).
Axes of the slice: x: 2, y: 2, z: 4, core: 2. Of those that a mesh axis runs over, the one named last changes fastest.
Arguments:
- snapshots: bfloat16 [8, 8, 4, 2048, 512], P('gx', 'gy'), may hold values from -120 to 120
- basis: bfloat16 [8, 8, 4, 24, 2048], P('gx', 'gy'), may hold values from -0.0625 to 0.0625
- node_counts: int32 [8, 8], P('gx', 'gy'), may hold values from 1024 to 2048, as said below
- adjacency: int32 [8, 8, 3], P('gx', 'gy'), may hold values from 0 to 63, as said below
Outputs:
- operator: float32 [8, 8, 397, 24], P('gx', 'gy')
- reduced_states: float32 [8, 8, 24, 512], P('gx', 'gy')
The draws below stay inside these ranges and needn't reach their ends.
Inputs may be any that keep to these rules, and one draw needn't show every extreme that they name: Node slot n of subdomain g is live iff n < node_counts[g]; at least 1024 slots are live, and one subdomain has all 2048 live. Subdomain (row, col) has id row * 8 + col. Each row of adjacency holds 3 distinct ids other than its own subdomain's, each within one subdomain row and one subdomain column of it.
All inputs are finite; a program needn't handle non-finite values.
Results may differ from the reference program's by a relative error of at most 0.0003.
Values sent between devices are 32-bit elements; how exact they have to be, the bound alone decides.
A program may use at most 64 MiB of HBM per device.

```python
import jax
import jax.numpy as jnp
import numpy as np
from jax import lax

R = 24
NVAR = 4
K = 512
P_SIZE = 2048
NB = 3
GRID_R = 8
GRID_C = 8
NF = 397


def draw_node_counts(key, part):
    first, second = jax.random.split(jax.random.fold_in(key, 11))
    counts = jax.random.randint(first, (GRID_R * GRID_C,), P_SIZE // 2, P_SIZE + 1, dtype=jnp.int32)
    where_full = jax.random.randint(second, (), 0, GRID_R * GRID_C, dtype=jnp.int32)
    counts = jnp.where(jnp.arange(GRID_R * GRID_C, dtype=jnp.int32) == where_full, P_SIZE, counts)
    return counts.reshape(GRID_R, GRID_C).astype(jnp.int32)


def draw_adjacency(key, part):
    offsets = np.array([(a, b) for a in range(-1, 2) for b in range(-1, 2)], dtype=np.int32)
    rows = jnp.arange(GRID_R, dtype=jnp.int32)[:, None, None]
    cols = jnp.arange(GRID_C, dtype=jnp.int32)[None, :, None]
    near_rows = jnp.broadcast_to(rows + jnp.asarray(offsets[:, 0]), (GRID_R, GRID_C, 9))
    near_cols = jnp.broadcast_to(cols + jnp.asarray(offsets[:, 1]), (GRID_R, GRID_C, 9))
    inside = (near_rows >= 0) & (near_rows < GRID_R) & (near_cols >= 0) & (near_cols < GRID_C)
    itself = (near_rows == rows) & (near_cols == cols)
    scores = jax.random.randint(jax.random.fold_in(key, 13), (GRID_R, GRID_C, 9), 0, 1000, dtype=jnp.int32) * 16 + jnp.arange(9, dtype=jnp.int32)
    scores = jnp.where(inside & jnp.logical_not(itself), scores, -1)
    unused, picked = lax.top_k(scores, NB)
    chosen_rows = jnp.take_along_axis(near_rows, picked, axis=2)
    chosen_cols = jnp.take_along_axis(near_cols, picked, axis=2)
    return (chosen_rows * GRID_C + chosen_cols).astype(jnp.int32)


def draw_snapshots(key, part):
    keys = jax.random.split(jax.random.fold_in(key, 17), 3)
    shape = (GRID_R, GRID_C, NVAR, P_SIZE, K)
    ident = jnp.arange(GRID_R * GRID_C, dtype=jnp.float32).reshape(GRID_R, GRID_C) / max(GRID_R * GRID_C - 1, 1)
    var_scale = jnp.exp(jax.random.uniform(keys[0], (NVAR,), jnp.float32, jnp.log(0.5), jnp.log(4.0)))
    rough = jax.random.uniform(keys[1], (GRID_R, GRID_C, NVAR, P_SIZE, 1), jnp.float32, 0.5, 1.5)
    base = jnp.clip(jax.random.normal(keys[2], shape, jnp.float32), -6.0, 6.0)
    rise = 1.0 + 2.0 * ident
    values = base * rough * var_scale[None, None, :, None, None] * rise[:, :, None, None, None]
    return values.astype(jnp.bfloat16)


def shard_levels(rng, shape, shards, least, top_value):
    loudness, own = 1.0, jax.random.fold_in(rng, 6)
    for position, parts in shards:
        steps = jnp.exp(jax.random.uniform(jax.random.fold_in(own, position), (parts,), jnp.float32, least / len(shards), top_value / len(shards)))
        loudness = loudness * jnp.repeat(steps, shape[position] // parts).reshape([-1 if axis == position else 1 for axis in range(len(shape))])
    return loudness


def gaussian(own_key, shape, deviation, reach, cuts=(), kind=jnp.bfloat16):
    result = jax.random.normal(own_key, shape, jnp.float32) * deviation
    if len(cuts) > 0:
        result = shard_levels(own_key, shape, cuts, -0.22, 0.18) * result
    return jnp.clip(result, min=-reach, max=reach).astype(kind)


def setup_inputs(seed: int = 0) -> dict:
    seeds = jax.random.split(jax.random.key(seed), 5)
    return {
        "snapshots": draw_snapshots(jax.random.fold_in(seeds[4], 71), 0),
        "basis": gaussian(seeds[1], (GRID_R, GRID_C, NVAR, R, P_SIZE), (NVAR * P_SIZE) ** -0.5, 0.0625, ((0, 8), (1, 4))),
        "node_counts": draw_node_counts(jax.random.fold_in(seeds[4], 71), 0),
        "adjacency": draw_adjacency(jax.random.fold_in(seeds[4], 71), 0),
    }


beta_linear = 0.5
beta_quad = 0.5

def project_one(items):
    values, modes, count = items
    live = (jnp.arange(values.shape[1], dtype=jnp.int32) < count).astype(jnp.float32)
    masked = modes.astype(jnp.float32) * live[None, None, :]
    proj = jnp.einsum('vrp,vpk->vrk', masked, values.astype(jnp.float32), precision=lax.Precision.HIGHEST)
    valf = values.astype(jnp.float32)
    squares = lax.optimization_barrier(jnp.sum(valf * valf * live[None, :, None], axis=(1, 2)))
    return (proj, squares)

def build_features(state, near):
    ranks = state.shape[0]
    steps = state.shape[1]
    pieces = [jnp.ones((1, steps), jnp.float32), state, near.reshape(-1, steps)]
    for first in range(ranks):
        pieces.append(state[first:first + 1] * state[first:])
    return jnp.concatenate(pieces, axis=0)

def fit_one(state, near, reg_diag):
    feats = build_features(state, near)
    past = feats[:, :-1]
    gram = jnp.dot(past, past.T, precision=lax.Precision.HIGHEST) + jnp.diag(reg_diag)
    rhs = jnp.dot(past, state[:, 1:].T, precision=lax.Precision.HIGHEST)
    factor = jnp.linalg.cholesky(gram)
    middle = jax.scipy.linalg.solve_triangular(factor, rhs, lower=True)
    return jax.scipy.linalg.solve_triangular(factor, middle, lower=True, trans=1)

def reference(snapshots, basis, node_counts, adjacency):
    grid_rows, grid_cols = (snapshots.shape[0], snapshots.shape[1])
    total = grid_rows * grid_cols
    values = snapshots.reshape(total, NVAR, P_SIZE, K)
    modes = basis.reshape(total, NVAR, R, P_SIZE)
    counts = node_counts.reshape(total).astype(jnp.int32)
    proj, squares = lax.map(project_one, (values, modes, counts))
    nodes = jnp.sum(counts.astype(jnp.float32))
    scale = jnp.sqrt(lax.optimization_barrier(jnp.sum(squares, axis=0)) / (nodes * K) + 1e-06)
    states = lax.optimization_barrier(jnp.sum(proj / scale[None, :, None, None], axis=1))
    gnorm = jnp.sum(states * states) / (total * R * K)
    near = states[adjacency.reshape(total, NB).astype(jnp.int32)]
    nlin = 1 + R + NB * R
    nquad = R * (R + 1) // 2
    reg_diag = K * jnp.concatenate([jnp.full((nlin,), beta_linear, jnp.float32) * gnorm, jnp.full((nquad,), beta_quad, jnp.float32) * gnorm * gnorm])
    operator = lax.map(lambda items: fit_one(items[0], items[1], reg_diag), (states, near))
    return (operator.reshape(grid_rows, grid_cols, NF, R), states.reshape(grid_rows, grid_cols, R, K))
```

```python
import jax
import jax.numpy as jnp
from jax import lax
from jax.experimental import pallas as pl
from jax.experimental.pallas import tpu as pltpu
from jax.sharding import PartitionSpec as P

beta_linear = 0.5
beta_quad = 0.5
LANES = 128
SUB = 8
HIGH = lax.Precision.HIGHEST


def padded_2(cells, sides, width):
    for axis, dim in sides:
        count = lax.axis_size(axis)
        ends = count - 1
        head = lax.slice_in_dim(cells, 0, width, axis=dim)
        tail = lax.slice_in_dim(cells, cells.shape[dim] - width, cells.shape[dim], axis=dim)
        cells = jnp.concatenate(
            [
                lax.ppermute(tail, axis, [(i, (i + 1) % count) for i in range(ends)]),
                cells,
                lax.ppermute(head, axis, [((i + 1) % count, i) for i in range(ends)]),
            ],
            axis=dim,
        )
    return cells


def pick_rows(pieces, links):
    ids = jnp.arange(pieces.shape[0], dtype=jnp.int32)
    hits = (links[:, :, None] == ids[None, None, :]).astype(jnp.float32)
    return jnp.einsum("sbn,nrk->sbrk", hits, pieces, precision=lax.Precision.HIGHEST)


def spread_row(tile, row):
    return jnp.broadcast_to(tile[row : row + 1, :], tile.shape)


def spread_lane(tile, lane):
    if isinstance(lane, int):
        return jnp.broadcast_to(tile[:, lane : lane + 1], tile.shape)
    return jnp.take_along_axis(tile, jnp.full(tile.shape, lane, jnp.int32), axis=1)


def reduce_panel(tiles, base):
    sub = lax.broadcasted_iota(jnp.int32, (SUB, LANES), 0)
    lane = lax.broadcasted_iota(jnp.int32, (SUB, LANES), 1)
    inside = (lane >= base) & (lane < base + SUB)
    unit = (lane - base == sub).astype(jnp.float32)
    count = len(tiles)
    cols = [[spread_lane(t, base + j) for j in range(SUB)] for t in tiles]
    tiles = [jnp.where(inside, unit, t) for t in tiles]
    for j in range(SUB):
        for s in range(count):
            here = cols[s][j]
            inv = 1.0 / spread_row(here, j)
            row = spread_row(tiles[s], j) * inv
            tiles[s] = jnp.where(sub == j, row, tiles[s] - here * row)
            for i in range(j + 1, SUB):
                row = spread_row(cols[s][i], j) * inv
                cols[s][i] = jnp.where(sub == j, row, cols[s][i] - here * row)
    return tiles, inside


def clear_rows(tile, base, inside, rows):
    out = jnp.where(inside, 0.0, tile)
    terms = [spread_lane(tile, base + j) * rows[j] for j in range(SUB)]
    while len(terms) > 1:
        terms = [a + b for a, b in zip(terms[::2], terms[1::2])]
    return out - terms[0]


def mm(a, b):
    return jnp.dot(a, b, precision=HIGH, preferred_element_type=jnp.float32)


def mm_t(a, b):
    return lax.dot_general(
        a, b, (((1,), (1,)), ((), ())), precision=HIGH, preferred_element_type=jnp.float32
    )


def fit_kernel(nlin, gnorm_ref, state_ref, near_ref, out_ref, f_ref, tail_ref, m_ref, d_ref):
    subs, ranks, steps = state_ref.shape
    nf = out_ref.shape[1]
    pad = f_ref.shape[1]
    blocks = nf // LANES
    head = blocks * LANES
    rest = pad - head
    gnorm = gnorm_ref[0]
    keep = (lax.broadcasted_iota(jnp.int32, (1, steps), 1) < steps - 1).astype(jnp.float32)
    for s in range(subs):
        state = state_ref[s]
        past = state * keep
        f_ref[s, nf - nf % SUB : pad, :] = jnp.zeros((pad - nf + nf % SUB, steps), jnp.float32)
        f_ref[s, 0:1, :] = keep
        f_ref[s, 1 : 1 + ranks, :] = past
        f_ref[s, 1 + ranks : nlin, :] = near_ref[s] * keep
        at = nlin
        for first in range(ranks):
            f_ref[s, at : at + ranks - first, :] = past[first : first + 1] * state[first:]
            at += ranks - first
        tail_ref[s] = jnp.zeros(tail_ref.shape[1:], jnp.float32)
        tail_ref[s, 0:ranks, :] = pltpu.roll(state, steps - 1, 1)
        tail_ref[s, ranks : ranks + rest, :] = f_ref[s, head:pad, :]
    row = lax.broadcasted_iota(jnp.int32, (pad, head + LANES), 0)
    col = lax.broadcasted_iota(jnp.int32, (pad, head + LANES), 1)
    level = jnp.where(row < nlin, beta_linear * gnorm, beta_quad * gnorm * gnorm) * steps
    level = jnp.where(row < nf, level, 1.0)
    shift = jnp.where(row < head, 0, ranks)
    ridge = jnp.where(col == row + shift, level, 0.0)
    for s in range(subs):
        feats = f_ref[s]
        m_ref[s, :, 0:head] = mm_t(feats, f_ref[s, 0:head, :]) + ridge[:, 0:head]
        m_ref[s, :, head:] = mm_t(feats, tail_ref[s]) + ridge[:, head:]

    def block(k, carry):
        at = pl.multiple_of(k * LANES, LANES)
        for s in range(subs):
            d_ref[s] = m_ref[s, pl.ds(at, LANES), pl.ds(at, LANES)]

        def panel(p, carry):
            base = p * SUB
            here = pl.ds(pl.multiple_of(base, SUB), SUB)
            done, inside = reduce_panel([d_ref[s, here, :] for s in range(subs)], base)
            for s in range(subs):
                rows = [spread_row(done[s], j) for j in range(SUB)]
                for r in range(0, LANES, SUB):
                    d_ref[s, r : r + SUB, :] = clear_rows(d_ref[s, r : r + SUB, :], base, inside, rows)
                d_ref[s, here, :] = done[s]
            return carry

        lax.fori_loop(0, LANES // SUB, panel, 0)
        for s in range(subs):
            rows = mm(d_ref[s], m_ref[s, pl.ds(at, LANES), :])
            m_ref[s] = m_ref[s] - mm(m_ref[s, :, pl.ds(at, LANES)], rows)
            m_ref[s, pl.ds(at, LANES), :] = rows
        return carry

    lax.fori_loop(0, blocks, block, 0)
    groups = rest // SUB
    tiles = [[m_ref[s, head + SUB * g : head + SUB * g + SUB, head:] for g in range(groups)] for s in range(subs)]
    for p in range(groups):
        base = ranks + p * SUB
        done, inside = reduce_panel([tiles[s][p] for s in range(subs)], base)
        for s in range(subs):
            rows = [spread_row(done[s], j) for j in range(SUB)]
            tiles[s] = [done[s] if g == p else clear_rows(tiles[s][g], base, inside, rows) for g in range(groups)]
    for s in range(subs):
        last = jnp.concatenate(tiles[s], axis=0)
        known = m_ref[s, 0:head, head:]
        out_ref[s, 0:head, :] = (known - mm(known[:, ranks : ranks + rest], last))[:, 0:ranks]
        out_ref[s, head:nf, :] = last[0 : nf - head, 0:ranks]


def fit(gnorm, states, near):
    subs, ranks, steps = states.shape
    nlin = 1 + ranks + near.shape[1]
    nf = nlin + ranks * (ranks + 1) // 2
    pad = -(-nf // SUB) * SUB
    head = nf // LANES * LANES

    def kernel(*refs):
        fit_kernel(nlin, *refs)

    vmem = pl.BlockSpec(memory_space=pltpu.VMEM)
    return pl.pallas_call(
        kernel,
        out_shape=jax.ShapeDtypeStruct((subs, nf, ranks), jnp.float32),
        in_specs=[pl.BlockSpec(memory_space=pltpu.SMEM), vmem, vmem],
        out_specs=vmem,
        scratch_shapes=[
            pltpu.VMEM((subs, pad, steps), jnp.float32),
            pltpu.VMEM((subs, LANES, steps), jnp.float32),
            pltpu.VMEM((subs, pad, head + LANES), jnp.float32),
            pltpu.VMEM((subs, LANES, LANES), jnp.float32),
        ],
        compiler_params=pltpu.CompilerParams(vmem_limit_bytes=40 * 2**20),
        name="fit",
    )(gnorm.reshape(1), states, near)


def body(snapshots, basis, node_counts, adjacency):
    values = snapshots[0]
    modes = basis[0]
    counts = node_counts[0]
    links = adjacency[0]
    columns = values.shape[0]
    slots = values.shape[2]
    steps = values.shape[3]
    ranks = modes.shape[2]
    live = jnp.arange(slots, dtype=jnp.int32)[None, :] < counts[:, None]
    masked = modes * live.astype(jnp.bfloat16)[:, None, None, :]
    proj = jnp.einsum("svrp,svpk->svrk", masked, values, preferred_element_type=jnp.float32)
    slotsq = jnp.einsum("svpk,svpk->svp", values, values, preferred_element_type=jnp.float32)
    squares = jnp.sum(slotsq * live.astype(jnp.float32)[:, None, :], axis=(0, 2))
    nodes = jnp.sum(counts.astype(jnp.float32))
    total_subs = lax.axis_size("gx") * lax.axis_size("gy") * columns
    grid_cols = columns * lax.axis_size("gy")
    near_row = links // grid_cols
    near_col = links % grid_cols
    local = (near_row - lax.axis_index("gx") + 1) * (columns + 2) + (
        near_col - lax.axis_index("gy") * columns + 1
    )
    cross = jnp.einsum("svrk,swrk->vw", proj, proj, precision=lax.Precision.HIGHEST)
    sq_all, nodes_all, cross_all = lax.psum((squares, nodes, cross), ("gx", "gy"))
    scale = jnp.sqrt(sq_all / (nodes_all * steps) + 1e-06)
    states = jnp.sum(proj / scale[None, :, None, None], axis=1)
    gnorm = jnp.sum(cross_all / (scale[:, None] * scale[None, :])) / (total_subs * ranks * steps)
    padded = padded_2(states[None], (("gx", 0), ("gy", 1)), 1)
    flat = padded.reshape(-1, ranks, steps)
    near = pick_rows(flat, local)
    operator = fit(gnorm, states, near.reshape(columns, -1, steps))
    return (operator[None], states[None])


def solution(mesh):
    in_specs = (
        P("gx", "gy", None, None, None),
        P("gx", "gy", None, None, None),
        P("gx", "gy"),
        P("gx", "gy", None),
    )
    out_specs = (P("gx", "gy", None, None), P("gx", "gy", None, None))
    return jax.shard_map(body, mesh=mesh, in_specs=in_specs, out_specs=out_specs, check_vma=False)
```

```python
import jax
import jax.numpy as jnp
from jax import lax
from jax.experimental import pallas as pl
from jax.experimental.pallas import tpu as pltpu
from jax.sharding import PartitionSpec as P

beta_linear = 0.5
beta_quad = 0.5
LANES = 128
SUB = 8
HIGH = lax.Precision.HIGHEST


def spread_row(tile, row):
    return jnp.broadcast_to(tile[row : row + 1, :], tile.shape)


def spread_lane(tile, lane):
    if isinstance(lane, int):
        return jnp.broadcast_to(tile[:, lane : lane + 1], tile.shape)
    return jnp.take_along_axis(tile, jnp.full(tile.shape, lane, jnp.int32), axis=1)


def reduce_panel(tiles, base):
    sub = lax.broadcasted_iota(jnp.int32, (SUB, LANES), 0)
    lane = lax.broadcasted_iota(jnp.int32, (SUB, LANES), 1)
    inside = (lane >= base) & (lane < base + SUB)
    unit = (lane - base == sub).astype(jnp.float32)
    count = len(tiles)
    cols = [[spread_lane(t, base + j) for j in range(SUB)] for t in tiles]
    tiles = [jnp.where(inside, unit, t) for t in tiles]
    for j in range(SUB):
        for s in range(count):
            here = cols[s][j]
            inv = 1.0 / spread_row(here, j)
            row = spread_row(tiles[s], j) * inv
            tiles[s] = jnp.where(sub == j, row, tiles[s] - here * row)
            for i in range(j + 1, SUB):
                row = spread_row(cols[s][i], j) * inv
                cols[s][i] = jnp.where(sub == j, row, cols[s][i] - here * row)
    return tiles, inside


def clear_rows(tile, base, inside, rows):
    out = jnp.where(inside, 0.0, tile)
    terms = [spread_lane(tile, base + j) * rows[j] for j in range(SUB)]
    while len(terms) > 1:
        terms = [a + b for a, b in zip(terms[::2], terms[1::2])]
    return out - terms[0]


def mm(a, b):
    return jnp.dot(a, b, precision=HIGH, preferred_element_type=jnp.float32)


def mm_t(a, b):
    return lax.dot_general(
        a, b, (((1,), (1,)), ((), ())), precision=HIGH, preferred_element_type=jnp.float32
    )


def fit_kernel(nlin, gnorm_ref, state_ref, near_ref, out_ref, kept_ref, f_ref, tail_ref, m_ref, d_ref):
    subs, ranks, steps = state_ref.shape
    nf = out_ref.shape[1]
    pad = f_ref.shape[1]
    blocks = nf // LANES
    head = blocks * LANES
    rest = pad - head
    gnorm = gnorm_ref[0:1, 0:1]
    kept_ref[...] = state_ref[...]
    keep = (lax.broadcasted_iota(jnp.int32, (1, steps), 1) < steps - 1).astype(jnp.float32)
    for s in range(subs):
        state = state_ref[s]
        past = state * keep
        f_ref[s, nf - nf % SUB : pad, :] = jnp.zeros((pad - nf + nf % SUB, steps), jnp.float32)
        f_ref[s, 0:1, :] = keep
        f_ref[s, 1 : 1 + ranks, :] = past
        f_ref[s, 1 + ranks : nlin, :] = near_ref[s] * keep
        at = nlin
        for first in range(ranks):
            f_ref[s, at : at + ranks - first, :] = past[first : first + 1] * state[first:]
            at += ranks - first
        tail_ref[s] = jnp.zeros(tail_ref.shape[1:], jnp.float32)
        tail_ref[s, 0:ranks, :] = pltpu.roll(state, steps - 1, 1)
        tail_ref[s, ranks : ranks + rest, :] = f_ref[s, head:pad, :]
    row = lax.broadcasted_iota(jnp.int32, (pad, head + LANES), 0)
    col = lax.broadcasted_iota(jnp.int32, (pad, head + LANES), 1)
    level = jnp.where(row < nlin, beta_linear * gnorm, beta_quad * gnorm * gnorm) * steps
    level = jnp.where(row < nf, level, 1.0)
    shift = jnp.where(row < head, 0, ranks)
    ridge = jnp.where(col == row + shift, level, 0.0)
    for s in range(subs):
        feats = f_ref[s]
        m_ref[s, :, 0:head] = mm_t(feats, f_ref[s, 0:head, :]) + ridge[:, 0:head]
        m_ref[s, :, head:] = mm_t(feats, tail_ref[s]) + ridge[:, head:]

    def block(k, carry):
        at = pl.multiple_of(k * LANES, LANES)
        for s in range(subs):
            d_ref[s] = m_ref[s, pl.ds(at, LANES), pl.ds(at, LANES)]

        def panel(p, carry):
            base = p * SUB
            here = pl.ds(pl.multiple_of(base, SUB), SUB)
            done, inside = reduce_panel([d_ref[s, here, :] for s in range(subs)], base)
            for s in range(subs):
                rows = [spread_row(done[s], j) for j in range(SUB)]
                for r in range(0, LANES, SUB):
                    d_ref[s, r : r + SUB, :] = clear_rows(d_ref[s, r : r + SUB, :], base, inside, rows)
                d_ref[s, here, :] = done[s]
            return carry

        lax.fori_loop(0, LANES // SUB, panel, 0)
        for s in range(subs):
            rows = mm(d_ref[s], m_ref[s, pl.ds(at, LANES), :])
            m_ref[s] = m_ref[s] - mm(m_ref[s, :, pl.ds(at, LANES)], rows)
            m_ref[s, pl.ds(at, LANES), :] = rows
        return carry

    lax.fori_loop(0, blocks, block, 0)
    groups = rest // SUB
    tiles = [[m_ref[s, head + SUB * g : head + SUB * g + SUB, head:] for g in range(groups)] for s in range(subs)]
    for p in range(groups):
        base = ranks + p * SUB
        done, inside = reduce_panel([tiles[s][p] for s in range(subs)], base)
        for s in range(subs):
            rows = [spread_row(done[s], j) for j in range(SUB)]
            tiles[s] = [done[s] if g == p else clear_rows(tiles[s][g], base, inside, rows) for g in range(groups)]
    for s in range(subs):
        last = jnp.concatenate(tiles[s], axis=0)
        known = m_ref[s, 0:head, head:]
        out_ref[s, 0:head, :] = (known - mm(known[:, ranks : ranks + rest], last))[:, 0:ranks]
        out_ref[s, head:nf, :] = last[0 : nf - head, 0:ranks]


def fit(gnorm, states, near):
    subs, ranks, steps = states.shape
    nlin = 1 + ranks + near.shape[1]
    nf = nlin + ranks * (ranks + 1) // 2
    pad = -(-nf // SUB) * SUB
    head = nf // LANES * LANES

    def kernel(*refs):
        fit_kernel(nlin, *refs)

    vmem = pl.BlockSpec(memory_space=pltpu.VMEM)
    return pl.pallas_call(
        kernel,
        out_shape=(
            jax.ShapeDtypeStruct((subs, nf, ranks), jnp.float32),
            jax.ShapeDtypeStruct(states.shape, jnp.float32),
        ),
        in_specs=[vmem, vmem, vmem],
        out_specs=(vmem, vmem),
        scratch_shapes=[
            pltpu.VMEM((subs, pad, steps), jnp.float32),
            pltpu.VMEM((subs, LANES, steps), jnp.float32),
            pltpu.VMEM((subs, pad, head + LANES), jnp.float32),
            pltpu.VMEM((subs, LANES, LANES), jnp.float32),
        ],
        compiler_params=pltpu.CompilerParams(vmem_limit_bytes=40 * 2**20),
        name="fit",
    )(gnorm, states, near)


def share_kernel(sizes, counts_ref, links_ref, proj_ref, slotsq_ref, near_ref, state_ref, gnorm_ref,
                 stat_ref, half_ref, row_ref, col_ref, cell_ref, row_sems, col_sems, halo_sems):
    nx, ny = sizes
    subs, nvar, ranks, steps = proj_ref.shape
    slots = slotsq_ref.shape[2]
    nbrs = links_ref.shape[1]
    x, y = lax.axis_index("gx"), lax.axis_index("gy")
    barrier = pltpu.get_barrier_semaphore()
    sides = [(dx, dy) for dx in (-1, 0, 1) for dy in (-1, 0, 1) if dx or dy]

    def at(dx, dy):
        return (lax.rem(x + dx + nx, nx), lax.rem(y + dy + ny, ny))

    greeted = [at(d, 0) for d in range(1, nx)] + [at(0, d) for d in range(1, ny)]
    greeted += [at(dx, dy) for dx, dy in sides if dx and dy]
    for other in greeted:
        pl.semaphore_signal(barrier, inc=1, device_id=other, device_id_type=pl.DeviceIdType.MESH)

    pairs = [(v, w) for v in range(nvar) for w in range(v, nvar)]
    lane = lax.broadcasted_iota(jnp.int32, (1, LANES), 1)
    stat_ref[...] = jnp.zeros(stat_ref.shape, jnp.float32)
    squares = jnp.zeros((nvar, LANES), jnp.float32)
    nodes = 0
    for s in range(subs):
        nodes = nodes + counts_ref[s]
        for p in range(0, slots, LANES):
            squares += jnp.where(lane + p < counts_ref[s], slotsq_ref[s, :, p : p + LANES], 0.0)
    stat_ref[0:nvar, :] = squares
    for i, (v, w) in enumerate(pairs):
        total = jnp.zeros((ranks, LANES), jnp.float32)
        for s in range(subs):
            for k in range(0, steps, LANES):
                total += proj_ref[s, v, :, k : k + LANES] * proj_ref[s, w, :, k : k + LANES]
        stat_ref[nvar + i : nvar + i + 1, :] = jnp.sum(total, axis=0, keepdims=True)
    last = nvar + len(pairs)
    stat_ref[last : last + 1, :] = jnp.where(lane == 0, nodes.astype(jnp.float32), 0.0)

    pl.semaphore_wait(barrier, len(greeted))

    def gather(src, slots_ref, sems, me, count, step):
        slots_ref[me] = src[...]
        copies = []
        for d in range(1, count):
            copies.append(
                pltpu.make_async_remote_copy(
                    src_ref=src,
                    dst_ref=slots_ref.at[me],
                    send_sem=sems.at[0, d],
                    recv_sem=sems.at[1, d],
                    device_id=step(d),
                    device_id_type=pl.DeviceIdType.MESH,
                )
            )
            copies[-1].start()
        for copy in copies:
            copy.wait_recv()
        total = slots_ref[0]
        for d in range(1, count):
            total = total + slots_ref[d]
        return total, copies

    half, sent = gather(stat_ref, row_ref, row_sems, x, nx, lambda d: at(d, 0))
    half_ref[...] = half
    total, more = gather(half_ref, col_ref, col_sems, y, ny, lambda d: at(0, d))
    sent += more
    total = jnp.broadcast_to(jnp.sum(total, axis=1, keepdims=True), total.shape)
    nodes = total[last : last + 1, :]
    scale = [jnp.sqrt(total[v : v + 1, :] / (nodes * steps) + 1e-06) for v in range(nvar)]
    gnorm = jnp.zeros((1, LANES), jnp.float32)
    for i, (v, w) in enumerate(pairs):
        gnorm += (1.0 if v == w else 2.0) * total[nvar + i : nvar + i + 1, :] / (scale[v] * scale[w])
    gnorm = gnorm / (nx * ny * subs * ranks * steps)
    gnorm_ref[...] = jnp.broadcast_to(gnorm, gnorm_ref.shape)
    inverse = [1.0 / part[:, 0:1] for part in scale]
    wide = subs + 2
    for s in range(subs):
        state = proj_ref[s, 0] * inverse[0]
        for v in range(1, nvar):
            state = state + proj_ref[s, v] * inverse[v]
        state_ref[s] = state
        cell_ref[wide + 1 + s] = state
    for i, (dx, dy) in enumerate(sides):
        first, size = (0, subs) if dy == 0 else ((subs - 1, 1) if dy > 0 else (0, 1))
        into = (1 - dx) * wide + (1 if dy == 0 else (0 if dy > 0 else subs + 1))
        copy = pltpu.make_async_remote_copy(
            src_ref=cell_ref.at[pl.ds(wide + 1 + first, size)],
            dst_ref=cell_ref.at[pl.ds(into, size)],
            send_sem=halo_sems.at[0, i],
            recv_sem=halo_sems.at[1, i],
            device_id=at(dx, dy),
            device_id_type=pl.DeviceIdType.MESH,
        )
        copy.start()
        sent.append(copy)
    for i, (dx, dy) in enumerate(sides):
        sent[len(sent) - len(sides) + i].wait_recv()
    for copy in sent:
        copy.wait_send()
    columns = ny * subs
    for s in range(subs):
        for b in range(nbrs):
            link = links_ref[s, b]
            row = link // columns
            cell = (row - x + 1) * wide + link - row * columns - y * subs + 1
            cell = jnp.clip(cell, 0, 3 * wide - 1)
            near_ref[s, b * ranks : b * ranks + ranks, :] = cell_ref[cell]


def share(counts, links, proj, slotsq):
    nx, ny = lax.axis_size("gx"), lax.axis_size("gy")
    subs, nvar, ranks, steps = proj.shape
    rows = -(-(nvar + nvar * (nvar + 1) // 2 + 1) // SUB) * SUB
    smem = pl.BlockSpec(memory_space=pltpu.SMEM)
    vmem = pl.BlockSpec(memory_space=pltpu.VMEM)

    def kernel(*refs):
        share_kernel((nx, ny), *refs)

    return pl.pallas_call(
        kernel,
        out_shape=(
            jax.ShapeDtypeStruct((subs, links.shape[1] * ranks, steps), jnp.float32),
            jax.ShapeDtypeStruct((subs, ranks, steps), jnp.float32),
            jax.ShapeDtypeStruct((SUB, LANES), jnp.float32),
        ),
        in_specs=[smem, smem, vmem, vmem],
        out_specs=(vmem, vmem, vmem),
        scratch_shapes=[
            pltpu.VMEM((rows, LANES), jnp.float32),
            pltpu.VMEM((rows, LANES), jnp.float32),
            pltpu.VMEM((nx, rows, LANES), jnp.float32),
            pltpu.VMEM((ny, rows, LANES), jnp.float32),
            pltpu.VMEM((3 * (subs + 2), ranks, steps), jnp.float32),
            pltpu.SemaphoreType.DMA((2, nx)),
            pltpu.SemaphoreType.DMA((2, ny)),
            pltpu.SemaphoreType.DMA((2, 8)),
        ],
        compiler_params=pltpu.CompilerParams(collective_id=0, has_side_effects=True),
        name="share",
    )(counts, links, proj, slotsq)


def body(snapshots, basis, node_counts, adjacency):
    values = snapshots[0]
    modes = basis[0]
    counts = node_counts[0]
    slots = values.shape[2]
    live = jnp.arange(slots, dtype=jnp.int32)[None, :] < counts[:, None]
    masked = modes * live.astype(jnp.bfloat16)[:, None, None, :]
    proj = jnp.einsum("svrp,svpk->svrk", masked, values, preferred_element_type=jnp.float32)
    slotsq = jnp.einsum("svpk,svpk->svp", values, values, preferred_element_type=jnp.float32)
    near, states, gnorm = share(counts, adjacency[0], proj, slotsq)
    operator, states = fit(gnorm, states, near)
    return (operator[None], states[None])


def solution(mesh):
    in_specs = (
        P("gx", "gy", None, None, None),
        P("gx", "gy", None, None, None),
        P("gx", "gy"),
        P("gx", "gy", None),
    )
    out_specs = (P("gx", "gy", None, None), P("gx", "gy", None, None))
    return jax.shard_map(body, mesh=mesh, in_specs=in_specs, out_specs=out_specs, check_vma=False)
```
